32 devices in a mesh: groups: 2 (over y), beam: 8 (over z, x), mp: 2 (over core).
Axes of the slice: x: 2, y: 2, z: 4, core: 2. Of those that a mesh axis runs over, the one named last changes fastest.
Arguments:
- states: float32 [64, 8, 128, 128], P(('groups', 'beam'), 'mp'), parts along dimension 0, may hold values from -4 to 4
- parent_beam: int32 [64], P(('groups', 'beam')), parts along dimension 0, may hold values from 0 to 7, as said below
- next_token: int32 [64], P(('groups', 'beam')), parts along dimension 0, may hold values from 0 to 1023
- proj_table: bfloat16 [1024, 8, 640], P('beam', 'mp'), may hold values from -6 to 6
- gate_table: bfloat16 [1024, 3, 8], P('beam', None, 'mp'), may hold values from -6 to 6
- gain: float32 [8, 128], P('mp'), may hold values from 0.1 to 1.9
Outputs:
- readout: bfloat16 [64, 8, 128], P(('groups', 'beam'), 'mp'), parts along dimension 0
- new_states: float32 [64, 8, 128, 128], P(('groups', 'beam'), 'mp'), parts along dimension 0
The draws below stay inside these ranges and needn't reach their ends.
There are 2 independent parts, one for each index of `groups`. The reference program is written for one: setup_inputs(seed, part) draws one part's arguments, and reference() takes and returns one part's arrays. A program takes and returns all parts, laid end to end along the dimension named above; an argument that names none is the same for every part. Nothing has to cross between parts.
Inputs may be any that keep to these rules, and one draw needn't show every extreme that they name: The parent of hypothesis h = b * 4 + u is parent_beam[h] * 4 + u. In each aligned block of 4 hypotheses at most 2 take their parent from any one beam other than their own beam, and every block has a beam that supplies exactly 2.
All inputs are finite; a program needn't handle non-finite values.
Results may differ from the reference program's by a relative error of at most 0.001.
Values may be sent and summed in bfloat16 or wider, within the bound.
A program may use at most 64 MiB of HBM per device.

```python
import math
import jax
import jax.numpy as jnp
import numpy as np
from jax import lax

HEADS = 8
HEAD_DIM = 128
BEAMS = 8
CAP = 2
HYP_DEV = 4
HYPS = 32
UTTS = 4
VOCAB = 1024


def draw_parent_beam(key, part):
    block_count = HYPS // HYP_DEV

    def draw_block(block_key, block_index):
        key_forced, key_pool, key_place = jax.random.split(block_key, 3)
        forced = jax.random.randint(key_forced, (), 1, BEAMS)
        offset_pool = jnp.concatenate([jnp.zeros((HYP_DEV,), jnp.int32), jnp.repeat(jnp.arange(1, BEAMS, dtype=jnp.int32), CAP)])
        shuffled = offset_pool[jax.random.permutation(key_pool, offset_pool.shape[0])]
        ordering = jnp.argsort((shuffled == forced).astype(jnp.int32), stable=True)
        remaining = shuffled[ordering][:HYP_DEV - CAP]
        offsets = jnp.concatenate([jnp.full((CAP,), forced, jnp.int32), remaining])
        offsets = offsets[jax.random.permutation(key_place, HYP_DEV)]
        own_beam = block_index * HYP_DEV // UTTS
        return ((own_beam - offsets) % BEAMS).astype(jnp.int32)
    block_keys = jax.random.split(jax.random.fold_in(key, 11), block_count)
    drawn = jax.vmap(draw_block)(block_keys, jnp.arange(block_count, dtype=jnp.int32))
    return drawn.reshape(HYPS).astype(jnp.int32)


def plant(values, rng, low, high):
    extent = values.shape
    place = [jax.random.randint(jax.random.fold_in(rng, axis), (), 0, extent[axis]) for axis in range(len(extent))]
    values = values.at[tuple(place)].set(low)
    longest = extent.index(max(extent))
    place[longest] = (place[longest] + 1) % extent[longest]
    return values.at[tuple(place)].set(high)


def block_levels(key, extent, shards, smallest, largest):
    level = 1.0
    for axis_at, blocks in shards:
        draws = jax.random.uniform(jax.random.fold_in(jax.random.fold_in(key, 6), axis_at), (blocks,), jnp.float32, smallest / len(shards), largest / len(shards))
        level = level * jnp.repeat(jnp.exp(draws), extent[axis_at] // blocks).reshape((-1,) + (1,) * (len(extent) - 1 - axis_at))
    return level


def rank_table(amount, lean):
    loads = [(1 << 20) // math.isqrt(grade ** lean) + 1 for grade in range(1, amount + 1)]
    deviation = 1 + sum(loads) // (1 << 30)
    return np.cumsum(np.array([max(1, weight // deviation) for weight in loads]))


def ranked_ids(key, dims, amount, slope):
    table = rank_table(amount, slope)
    ticket = jax.random.randint(jax.random.fold_in(key, 1), dims, 0, int(table[amount - 1]))
    grade = jnp.searchsorted(jnp.asarray(table, jnp.int32), ticket, side="right")
    return jax.random.permutation(jax.random.fold_in(key, 2), amount)[grade].astype(jnp.int32)


def gaussian(rng, extent, spread, limit, cuts=(), kind=jnp.bfloat16):
    level = block_levels(rng, extent, cuts, -0.22, 0.18) if cuts else 1.0
    values = jax.random.normal(rng, extent, jnp.float32) * spread * level
    return jnp.minimum(jnp.maximum(values, -limit), limit).astype(kind)


def setup_inputs(seed: int = 0, part: int = 0) -> dict:
    key_of = jax.random.split(jax.random.key(seed), 7)
    part_keys = jax.random.split(jax.random.fold_in(key_of[6], part), 7)
    states = gaussian(part_keys[0], (HYPS, HEADS, HEAD_DIM, HEAD_DIM), 0.5, 4.0, ((0, 8), (1, 2)), jnp.float32)
    parent_beam = draw_parent_beam(jax.random.fold_in(jax.random.fold_in(key_of[6], part), 71), part)
    next_token = plant(ranked_ids(part_keys[2], (HYPS,), VOCAB, 2), jax.random.fold_in(part_keys[2], 3), 0, VOCAB - 1).astype(jnp.int32)
    proj_table = gaussian(key_of[3], (VOCAB, HEADS, 5 * HEAD_DIM), 1.0, 6.0, ((0, 8), (1, 2)))
    gate_table = gaussian(key_of[4], (VOCAB, 3, HEADS), 1.5, 6.0, ((0, 8), (2, 2)))
    gain = jnp.clip(1.0 + 0.18 * jax.random.normal(key_of[5], (HEADS, HEAD_DIM), jnp.float32), 0.1, 1.9)
    return dict(states=states, parent_beam=parent_beam, next_token=next_token, proj_table=proj_table, gate_table=gate_table, gain=gain)


def unit_norm(vector):
    return vector * lax.rsqrt(lax.optimization_barrier(jnp.sum(vector * vector, axis=-1, keepdims=True)) + 1e-06)

def advance(parents, entries, gate_entries, gain):
    retain = jax.nn.sigmoid(gate_entries[:, 0, :])
    strengths = 2.0 * jax.nn.sigmoid(gate_entries[:, 1:, :])
    state_now = retain[:, :, None, None] * parents
    for reflect in range(2):
        key_unit = unit_norm(entries[:, :, 1 + reflect, :])
        value_row = entries[:, :, 3 + reflect, :]
        applied = jnp.einsum('nhvd,nhd->nhv', state_now, key_unit, precision=lax.Precision.HIGHEST)
        state_now = state_now - strengths[:, reflect, :, None, None] * (applied - value_row)[:, :, :, None] * key_unit[:, :, None, :]
    query_unit = unit_norm(entries[:, :, 0, :])
    readout = jnp.einsum('nhvd,nhd->nhv', state_now, query_unit, precision=lax.Precision.HIGHEST)
    normed = gain[None, :, :] * readout * lax.rsqrt(lax.optimization_barrier(jnp.mean(readout * readout, axis=-1, keepdims=True)) + 1e-05)
    return (normed.astype(jnp.bfloat16), state_now)

def reference(states, parent_beam, next_token, proj_table, gate_table, gain):
    hyp_index = jnp.arange(HYPS, dtype=jnp.int32)
    utterance = hyp_index % UTTS
    parent_hyp = (parent_beam * UTTS + utterance).astype(jnp.int32)
    parents = states[parent_hyp]
    entries = proj_table[next_token].astype(jnp.float32).reshape(HYPS, HEADS, 5, HEAD_DIM)
    gate_entries = gate_table[next_token].astype(jnp.float32)
    return advance(parents, entries, gate_entries, gain)
```

```python
import jax
import jax.numpy as jnp
from jax import lax
from jax.experimental import pallas as pl
from jax.experimental.pallas import tpu as pltpu
from jax.sharding import PartitionSpec as P

HEAD_DIM = 128
BEAMS = 8
SPLIT = 2
AHEAD = 2
PEAK = 4.0
LEVELS = 32767.0
MESH = pl.DeviceIdType.MESH


def encode(x):
    root = jnp.sqrt(jnp.sqrt(jnp.sqrt(jnp.abs(x) * (1.0 / PEAK))))
    scaled = jnp.where(x < 0, -root, root) * LEVELS
    return jnp.round(scaled).astype(jnp.int32).astype(jnp.int16)


def decode(code):
    y = code.astype(jnp.int32).astype(jnp.float32) * (1.0 / LEVELS)
    y2 = y * y
    y4 = y2 * y2
    return (y4 * PEAK) * (y4 * jnp.where(y < 0, -1.0, 1.0))


def flip(beam, bit):
    return beam + bit - 2 * bit * lax.rem(lax.div(beam, bit), 2)


def exchange_kernel(
    n, heads, hyps, vocab, states, meta, table, picked, ent,
    own, mir, xsnd, xrcv, zsnd, zrcv, mrcv, esnd, ercv,
    send_sems, recv_sems, msend, mrecv, esend, erecv,
):
    me = lax.axis_index("beam")
    spacing = n // BEAMS
    beam = lax.div(me, spacing)
    off = lax.rem(me, spacing)

    def device(b):
        return b * spacing + off

    def peer(j):
        return lax.rem(me + j, n)

    chunks = heads * SPLIT
    rows = HEAD_DIM // SPLIT
    ids = hyps * heads

    barrier = pltpu.get_barrier_semaphore()
    for j in range(1, n):
        pl.semaphore_signal(barrier, inc=1, device_id={"beam": peer(j)}, device_id_type=MESH)

    for i in range(chunks):
        h, s = i // SPLIT, i % SPLIT
        for u in range(hyps):
            own[i, u] = encode(states[u, h, s * rows:(s + 1) * rows, :])

    pl.semaphore_wait(barrier, n - 1)

    def remote(src, dst, send, recv, to):
        return pltpu.make_async_remote_copy(
            src_ref=src, dst_ref=dst, send_sem=send, recv_sem=recv,
            device_id={"beam": to}, device_id_type=MESH,
        )

    metas = [None]
    for j in range(1, n):
        c = remote(meta, mrcv.at[j], msend.at[j], mrecv.at[j], peer(j))
        c.start()
        metas.append(c)

    across, beside, along = flip(beam, 4), flip(beam, 1), flip(beam, 2)
    diagonal = flip(beside, 2)
    first = [remote(own.at[i], mir.at[i], send_sems.at[0, i], recv_sems.at[0, i], device(across)) for i in range(chunks)]
    second = [remote(xsnd.at[i], xrcv.at[i], send_sems.at[1, i], recv_sems.at[1, i], device(beside)) for i in range(chunks)]
    third = [remote(zsnd.at[i], zrcv.at[i], send_sems.at[2, i], recv_sems.at[2, i], device(along)) for i in range(chunks)]
    for i in range(AHEAD):
        first[i].start()

    mrcv[0] = meta[...]
    for j in range(1, n):
        metas[j].wait()

    spot = lax.broadcasted_iota(jnp.int32, (ids, vocab), 1) + me * vocab
    head_of = lax.broadcasted_iota(jnp.int32, (ids, vocab), 0) // hyps
    entries = [None]
    for j in range(n):
        hit = mrcv[j, 0:ids, :] == spot
        found = jnp.zeros((ids, table.shape[2]), jnp.float32)
        for h in range(heads):
            mask = (hit & (head_of == h)).astype(jnp.float32).astype(jnp.bfloat16)
            found += jnp.dot(mask, table[h], preferred_element_type=jnp.float32)
        if j == 0:
            ercv[0] = found.astype(jnp.bfloat16)
        else:
            esnd[j] = found.astype(jnp.bfloat16)
            c = remote(esnd.at[j], ercv.at[j], esend.at[j], erecv.at[j], peer(n - j))
            c.start()
            entries.append(c)

    def parents_of(b):
        slot = lax.rem(me - device(b) + n, n)
        return mrcv[slot, ids:ids + hyps, :][:, :HEAD_DIM]

    mine = parents_of(beam)
    at_beside, at_diagonal, at_along = parents_of(beside), parents_of(diagonal), parents_of(along)

    def wide(code):
        return code.astype(jnp.int32)

    for i in range(chunks + 2):
        if i < chunks:
            first[i].wait_recv()
            if i + AHEAD < chunks:
                first[i + AHEAD].start()
            for u in range(hyps):
                a, m = wide(own[i, u]), wide(mir[i, u])
                xsnd[i, u] = jnp.where(at_beside[u:u + 1] == beam, a, m).astype(jnp.int16)
                xsnd[i, hyps + u] = jnp.where(at_diagonal[u:u + 1] == beam, a, m).astype(jnp.int16)
            second[i].start()
        if 1 <= i <= chunks:
            t = i - 1
            second[t].wait_recv()
            for u in range(hyps):
                a, m, x = wide(own[t, u]), wide(mir[t, u]), wide(xrcv[t, hyps + u])
                p = at_along[u:u + 1]
                zsnd[t, u] = jnp.where(p == beam, a, jnp.where(p == across, m, x)).astype(jnp.int16)
            third[t].start()
        if i >= 2:
            t = i - 2
            h, s = t // SPLIT, t % SPLIT
            third[t].wait_recv()
            for u in range(hyps):
                m, x, z = wide(mir[t, u]), wide(xrcv[t, u]), wide(zrcv[t, u])
                p = mine[u:u + 1]
                near = (p == beside) | (p == flip(beside, 4))
                got = jnp.where(p == across, m, jnp.where(near, x, z))
                picked[u, h, s * rows:(s + 1) * rows, :] = got.astype(jnp.int16)

    total = ercv[0].astype(jnp.float32)
    for j in range(1, n):
        entries[j].wait_recv()
        total += ercv[j].astype(jnp.float32)
    ent[...] = total
    for j in range(1, n):
        entries[j].wait_send()
    for i in range(chunks):
        first[i].wait_send()
        second[i].wait_send()
        third[i].wait_send()


def unit_norm(vector):
    return vector * lax.rsqrt(jnp.sum(vector * vector, axis=-1, keepdims=True) + 1e-06)


def update_kernel(heads, hyps, beams, states, picked, ent, gain, readout, new_states):
    d = HEAD_DIM
    query = unit_norm(ent[:, 0:d])
    keys = (unit_norm(ent[:, d:2 * d]), unit_norm(ent[:, 2 * d:3 * d]))
    values = (ent[:, 3 * d:4 * d].T, ent[:, 4 * d:5 * d].T)
    gates = jax.nn.sigmoid(ent[:, 5 * d:6 * d])
    lane = lax.broadcasted_iota(jnp.int32, (d, heads * hyps), 1)
    outs = jnp.zeros((d, heads * hyps), jnp.float32)
    my_beam = beams[hyps]
    for h in range(heads):
        for u in range(hyps):
            i = h * hyps + u
            now = jnp.where(beams[u] == my_beam, states[u, h], decode(picked[u, h]))
            now = gates[i:i + 1, 0:1] * now
            for j in range(2):
                key = keys[j][i:i + 1, :]
                applied = jnp.sum(now * key, axis=1, keepdims=True)
                step = (2.0 * gates[i:i + 1, 1 + j:2 + j]) * (applied - values[j][:, i:i + 1])
                now = now - step * key
            new_states[u, h] = now
            out = jnp.sum(now * query[i:i + 1, :], axis=1, keepdims=True)
            outs = jnp.where(lane == i, out, outs)
    rows = outs.T
    rows = rows * lax.rsqrt(jnp.mean(rows * rows, axis=-1, keepdims=True) + 1e-05)
    for h in range(heads):
        for u in range(hyps):
            i = h * hyps + u
            readout[u, h:h + 1, :] = (gain[h:h + 1, :] * rows[i:i + 1, :]).astype(jnp.bfloat16)


def local(states, parent_beam, next_token, proj_table, gate_table, gain):
    hyps, heads = states.shape[:2]
    vocab = proj_table.shape[0]
    n = lax.axis_size("beam")
    ids = hyps * heads
    my_beam = lax.axis_index("beam") // (n // BEAMS)
    chunks, rows = heads * SPLIT, HEAD_DIM // SPLIT
    column = jnp.concatenate([jnp.tile(next_token, heads), parent_beam, jnp.zeros((-(ids + hyps) % 8,), jnp.int32)])
    meta = jnp.broadcast_to(column[:, None], (column.shape[0], vocab))
    gates = jnp.pad(jnp.transpose(gate_table, (2, 0, 1)), ((0, 0), (0, 0), (0, HEAD_DIM - 3)))
    table = jnp.concatenate([jnp.transpose(proj_table, (1, 0, 2)), gates], axis=2)
    width = table.shape[2]
    vmem = pl.BlockSpec(memory_space=pltpu.VMEM)

    def codes(slots):
        return pltpu.VMEM((chunks, slots, rows, HEAD_DIM), jnp.int16)

    dma = pltpu.SemaphoreType.DMA
    picked, ent = pl.pallas_call(
        lambda *refs: exchange_kernel(n, heads, hyps, vocab, *refs),
        out_shape=(
            jax.ShapeDtypeStruct(states.shape, jnp.int16),
            jax.ShapeDtypeStruct((ids, width), jnp.float32),
        ),
        in_specs=[vmem] * 3,
        out_specs=(vmem, vmem),
        scratch_shapes=[
            codes(hyps), codes(hyps), codes(2 * hyps), codes(2 * hyps), codes(hyps), codes(hyps),
            pltpu.VMEM((n,) + meta.shape, jnp.int32),
            pltpu.VMEM((n, ids, width), jnp.bfloat16),
            pltpu.VMEM((n, ids, width), jnp.bfloat16),
            dma((3, chunks)), dma((3, chunks)), dma((n,)), dma((n,)), dma((n,)), dma((n,)),
        ],
        compiler_params=pltpu.CompilerParams(collective_id=0, has_side_effects=True),
        name="exchange",
    )(states, meta, table)
    beams = jnp.concatenate([parent_beam, my_beam[None].astype(jnp.int32)])
    return pl.pallas_call(
        lambda *refs: update_kernel(heads, hyps, refs[0], *refs[1:]),
        out_shape=(
            jax.ShapeDtypeStruct((hyps, heads, HEAD_DIM), jnp.bfloat16),
            jax.ShapeDtypeStruct(states.shape, jnp.float32),
        ),
        in_specs=[pl.BlockSpec(memory_space=pltpu.SMEM)] + [vmem] * 4,
        out_specs=(vmem, vmem),
        name="update",
    )(beams, states, picked, ent, gain)


def solution(mesh):
    return jax.shard_map(
        local,
        mesh=mesh,
        in_specs=(
            P(("groups", "beam"), "mp", None, None),
            P(("groups", "beam")),
            P(("groups", "beam")),
            P("beam", "mp", None),
            P("beam", None, "mp"),
            P("mp", None),
        ),
        out_specs=(P(("groups", "beam"), "mp", None), P(("groups", "beam"), "mp", None, None)),
        check_vma=False,
    )
```

```python
import jax
import jax.numpy as jnp
from jax import lax
from jax.experimental import pallas as pl
from jax.experimental.pallas import tpu as pltpu
from jax.sharding import PartitionSpec as P

HEAD_DIM = 128
BEAMS = 8
SPLIT = 2
AHEAD = 3
PEAK = 4.0
LEVELS = 32767.0
MESH = pl.DeviceIdType.MESH


def encode(x):
    root = jnp.sqrt(jnp.sqrt(jnp.sqrt(jnp.abs(x) * (1.0 / PEAK))))
    scaled = jnp.where(x < 0, -root, root) * LEVELS
    return jnp.round(scaled).astype(jnp.int32).astype(jnp.int16)


def decode(code):
    y = code.astype(jnp.int32).astype(jnp.float32) * (1.0 / LEVELS)
    y2 = y * y
    y4 = y2 * y2
    return (y4 * PEAK) * (y4 * jnp.where(y < 0, -1.0, 1.0))


def flip(beam, bit):
    return beam + bit - 2 * bit * lax.rem(lax.div(beam, bit), 2)


def unit_norm(vector):
    return vector * lax.rsqrt(jnp.sum(vector * vector, axis=-1, keepdims=True) + 1e-06)


def step_kernel(
    n, heads, hyps, vocab, states, token, parent, table, gate, gain, readout, new_states,
    held, own, mir, xsnd, xrcv, zsnd, zrcv, mloc, mrcv, esnd, ercv, fresh,
    send_sems, recv_sems, msend, mrecv, esend, erecv, load_sems, store_sems,
):
    me = lax.axis_index("beam")
    spacing = n // BEAMS
    beam = lax.div(me, spacing)
    off = lax.rem(me, spacing)
    d = HEAD_DIM

    def device(b):
        return b * spacing + off

    def peer(j):
        return lax.rem(me + j, n)

    chunks = heads * SPLIT
    rows = d // SPLIT
    ids = hyps * heads

    loads = [pltpu.make_async_copy(states.at[:, h], held.at[h], load_sems.at[h]) for h in range(heads)]
    for c in loads:
        c.start()
    barrier = pltpu.get_barrier_semaphore()
    for j in range(1, n):
        pl.semaphore_signal(barrier, inc=1, device_id={"beam": peer(j)}, device_id_type=MESH)

    mloc[...] = jnp.zeros(mloc.shape, jnp.int32)
    for h in range(heads):
        mloc[:, h * hyps:(h + 1) * hyps] = token[...] * heads + h
    mloc[:, ids:ids + hyps] = parent[...]

    def encode_head(h):
        loads[h].wait()
        for s in range(SPLIT):
            for u in range(hyps):
                own[h * SPLIT + s, u] = encode(held[h, u, s * rows:(s + 1) * rows, :])

    encode_head(0)
    pl.semaphore_wait(barrier, n - 1)

    def remote(src, dst, send, recv, to):
        return pltpu.make_async_remote_copy(
            src_ref=src, dst_ref=dst, send_sem=send, recv_sem=recv,
            device_id={"beam": to}, device_id_type=MESH,
        )

    metas = [None]
    for j in range(1, n):
        c = remote(mloc, mrcv.at[j], msend.at[j], mrecv.at[j], peer(j))
        c.start()
        metas.append(c)

    across, beside, along = flip(beam, 4), flip(beam, 1), flip(beam, 2)
    diagonal = flip(beside, 2)
    first = [remote(own.at[i], mir.at[i], send_sems.at[0, i], recv_sems.at[0, i], device(across)) for i in range(chunks)]
    second = [remote(xsnd.at[i], xrcv.at[i], send_sems.at[1, i], recv_sems.at[1, i], device(beside)) for i in range(chunks)]
    third = [remote(zsnd.at[i], zrcv.at[i], send_sems.at[2, i], recv_sems.at[2, i], device(along)) for i in range(chunks)]
    started = 0
    while started < min(AHEAD, SPLIT):
        first[started].start()
        started += 1
    for h in range(1, heads):
        encode_head(h)
        while started < min(AHEAD, (h + 1) * SPLIT):
            first[started].start()
            started += 1

    mrcv[0] = mloc[...]
    for j in range(1, n):
        metas[j].wait()

    keys_of = jnp.concatenate([mrcv[j] for j in range(n)], axis=0).T
    spot = lax.broadcasted_iota(jnp.int32, (ids, vocab * heads), 1) + me * (vocab * heads)
    gate_spot = lax.broadcasted_iota(jnp.int32, (ids, vocab), 1) + me * vocab
    head_of = lax.broadcasted_iota(jnp.int32, (ids, 1), 0) // hyps
    head_lane = lax.broadcasted_iota(jnp.int32, (ids, heads), 1) == head_of
    lane = lax.broadcasted_iota(jnp.int32, (ids, d), 1)
    flat = table[...].reshape(vocab * heads, 5 * d)
    entries = [None]
    for j in range(n):
        key = keys_of[0:ids, j:j + 1]
        hit = (key == spot).astype(jnp.float32).astype(jnp.bfloat16)
        found = jnp.dot(hit, flat, preferred_element_type=jnp.float32).astype(jnp.bfloat16)
        word = (key - head_of == gate_spot * heads).astype(jnp.float32).astype(jnp.bfloat16)
        gates = jnp.zeros((ids, d), jnp.float32)
        for g in range(3):
            every = lax.dot_general(word, gate[g], (((1,), (1,)), ((), ())), preferred_element_type=jnp.float32)
            one = jnp.sum(jnp.where(head_lane, every, 0.0), axis=1, keepdims=True)
            gates = jnp.where(lane == g, one, gates)
        to = ercv.at[0] if j == 0 else esnd.at[j]
        to[:, 0:5 * d] = found
        to[:, 5 * d:6 * d] = gates.astype(jnp.bfloat16)
        if j > 0:
            c = remote(esnd.at[j], ercv.at[j], esend.at[j], erecv.at[j], peer(n - j))
            c.start()
            entries.append(c)

    place = lax.broadcasted_iota(jnp.int32, (1, d), 1)

    def parents_of(b):
        row = mrcv[lax.rem(me - device(b) + n, n)]
        return [jnp.broadcast_to(jnp.sum(jnp.where(place == ids + u, row, 0), axis=1, keepdims=True), (1, d)) for u in range(hyps)]

    mine = parents_of(beam)
    at_beside, at_diagonal, at_along = parents_of(beside), parents_of(diagonal), parents_of(along)

    def wide(code):
        return code.astype(jnp.int32)

    stores = []
    outs = [jnp.zeros((rows, d), jnp.float32) for s in range(SPLIT)]
    out_lane = lax.broadcasted_iota(jnp.int32, (rows, d), 1)
    for i in range(chunks + 2):
        if i < chunks:
            first[i].wait_recv()
            if started < chunks:
                first[started].start()
                started += 1
            for u in range(hyps):
                a, m = wide(own[i, u]), wide(mir[i, u])
                xsnd[i, u] = jnp.where(at_beside[u] == beam, a, m).astype(jnp.int16)
                xsnd[i, hyps + u] = jnp.where(at_diagonal[u] == beam, a, m).astype(jnp.int16)
            second[i].start()
        if 1 <= i <= chunks:
            t = i - 1
            second[t].wait_recv()
            for u in range(hyps):
                a, m, x = wide(own[t, u]), wide(mir[t, u]), wide(xrcv[t, hyps + u])
                p = at_along[u]
                zsnd[t, u] = jnp.where(p == beam, a, jnp.where(p == across, m, x)).astype(jnp.int16)
            third[t].start()
        if i == 2:
            total = ercv[0].astype(jnp.float32)
            for j in range(1, n):
                entries[j].wait_recv()
                total += ercv[j].astype(jnp.float32)
            query = unit_norm(total[:, 0:d])
            keys = (unit_norm(total[:, d:2 * d]), unit_norm(total[:, 2 * d:3 * d]))
            values = (total[:, 3 * d:4 * d].T, total[:, 4 * d:5 * d].T)
            gates = jax.nn.sigmoid(total[:, 5 * d:6 * d])
        if i >= 2:
            t = i - 2
            h, s = t // SPLIT, t % SPLIT
            part = slice(s * rows, (s + 1) * rows)
            third[t].wait_recv()
            for u in range(hyps):
                m, x, z = wide(mir[t, u]), wide(xrcv[t, u]), wide(zrcv[t, u])
                p = mine[u]
                near = (p == beside) | (p == flip(beside, 4))
                got = decode(jnp.where(p == across, m, jnp.where(near, x, z)))
                k = h * hyps + u
                now = gates[k:k + 1, 0:1] * jnp.where(p == beam, held[h, u, part, :], got)
                for j in range(2):
                    key = keys[j][k:k + 1, :]
                    applied = jnp.sum(now * key, axis=1, keepdims=True)
                    now = now - (2.0 * gates[k:k + 1, 1 + j:2 + j]) * (applied - values[j][part, k:k + 1]) * key
                fresh[t, u] = now
                out = jnp.sum(now * query[k:k + 1, :], axis=1, keepdims=True)
                outs[s] = jnp.where(out_lane == k, out, outs[s])
            c = pltpu.make_async_copy(fresh.at[t], new_states.at[:, h, part, :], store_sems.at[t])
            c.start()
            stores.append(c)

    out_rows = jnp.concatenate(outs, axis=0).T[0:ids]
    out_rows = out_rows * lax.rsqrt(jnp.mean(out_rows * out_rows, axis=-1, keepdims=True) + 1e-05)
    for h in range(heads):
        for u in range(hyps):
            k = h * hyps + u
            readout[u, h:h + 1, :] = (gain[h:h + 1, :] * out_rows[k:k + 1, :]).astype(jnp.bfloat16)
    for j in range(1, n):
        entries[j].wait_send()
    for i in range(chunks):
        first[i].wait_send()
        second[i].wait_send()
        third[i].wait_send()
        stores[i].wait()


def local(states, parent_beam, next_token, proj_table, gate_table, gain):
    hyps, heads = states.shape[:2]
    vocab = proj_table.shape[0]
    n = lax.axis_size("beam")
    ids = hyps * heads
    chunks, rows = heads * SPLIT, HEAD_DIM // SPLIT
    width = 6 * HEAD_DIM
    vmem = pl.BlockSpec(memory_space=pltpu.VMEM)
    hbm = pl.BlockSpec(memory_space=pl.ANY)

    def codes(slots):
        return pltpu.VMEM((chunks, slots, rows, HEAD_DIM), jnp.int16)

    dma = pltpu.SemaphoreType.DMA
    return pl.pallas_call(
        lambda *refs: step_kernel(n, heads, hyps, vocab, *refs),
        out_shape=(
            jax.ShapeDtypeStruct((hyps, heads, HEAD_DIM), jnp.bfloat16),
            jax.ShapeDtypeStruct(states.shape, jnp.float32),
        ),
        in_specs=[hbm] + [vmem] * 5,
        out_specs=(vmem, hbm),
        scratch_shapes=[
            pltpu.VMEM((heads, hyps, HEAD_DIM, HEAD_DIM), jnp.float32),
            codes(hyps), codes(hyps), codes(2 * hyps), codes(2 * hyps), codes(hyps), codes(hyps),
            pltpu.VMEM((1, HEAD_DIM), jnp.int32),
            pltpu.VMEM((n, 1, HEAD_DIM), jnp.int32),
            pltpu.VMEM((n, ids, width), jnp.bfloat16),
            pltpu.VMEM((n, ids, width), jnp.bfloat16),
            pltpu.VMEM((chunks, hyps, rows, HEAD_DIM), jnp.float32),
            dma((3, chunks)), dma((3, chunks)), dma((n,)), dma((n,)), dma((n,)), dma((n,)),
            dma((heads,)), dma((chunks,)),
        ],
        compiler_params=pltpu.CompilerParams(collective_id=0, has_side_effects=True),
        name="step",
    )(
        states, next_token.reshape(1, hyps), parent_beam.reshape(1, hyps), proj_table,
        jnp.transpose(gate_table, (1, 2, 0)), gain,
    )


def solution(mesh):
    return jax.shard_map(
        local,
        mesh=mesh,
        in_specs=(
            P(("groups", "beam"), "mp", None, None),
            P(("groups", "beam")),
            P(("groups", "beam")),
            P("beam", "mp", None),
            P("beam", None, "mp"),
            P("mp", None),
        ),
        out_specs=(P(("groups", "beam"), "mp", None), P(("groups", "beam"), "mp", None, None)),
        check_vma=False,
    )
```

```python
import jax
import jax.numpy as jnp
from jax import lax
from jax.experimental import pallas as pl
from jax.experimental.pallas import tpu as pltpu
from jax.sharding import PartitionSpec as P

HEAD_DIM = 128
BEAMS = 8
SPLIT = 2
AHEAD = 3
LAG = 2
PEAK = 4.0
LEVELS = 32767.0
MESH = pl.DeviceIdType.MESH


def encode(x):
    root = jnp.sqrt(jnp.sqrt(jnp.sqrt(jnp.abs(x) * (1.0 / PEAK))))
    scaled = jnp.where(x < 0, -root, root) * LEVELS
    return jnp.round(scaled).astype(jnp.int32).astype(jnp.int16)


def decode(code):
    y = code.astype(jnp.int32).astype(jnp.float32) * (1.0 / LEVELS)
    y2 = y * y
    y4 = y2 * y2
    return (y4 * PEAK) * (y4 * jnp.where(y < 0, -1.0, 1.0))


def flip(beam, bit):
    return beam + bit - 2 * bit * lax.rem(lax.div(beam, bit), 2)


def unit_norm(vector):
    return vector * lax.rsqrt(jnp.sum(vector * vector, axis=-1, keepdims=True) + 1e-06)


def step_kernel(
    n, heads, hyps, vocab, states, token, parent, table, gate, gain, readout, new_states,
    held, own, mir, xsnd, xrcv, zsnd, zrcv, mloc, mrcv, esnd, ercv, fresh,
    keys, columns, strengths, outs,
    send_sems, recv_sems, msend, mrecv, esend, erecv, load_sems, store_sems,
):
    me = lax.axis_index("beam")
    spacing = n // BEAMS
    beam = lax.div(me, spacing)
    off = lax.rem(me, spacing)
    d = HEAD_DIM
    chunks = heads * SPLIT
    rows = d // SPLIT
    ids = hyps * heads

    def device(b):
        return b * spacing + off

    def peer(j):
        return lax.rem(me + j, n)

    def repeat(low, high, body):
        def step(i, carry):
            body(i)
            return carry
        lax.fori_loop(low, high, step, 0)

    def remote(src, dst, send, recv, to):
        return pltpu.make_async_remote_copy(
            src_ref=src, dst_ref=dst, send_sem=send, recv_sem=recv,
            device_id={"beam": to}, device_id_type=MESH,
        )

    across, beside, along = flip(beam, 4), flip(beam, 1), flip(beam, 2)
    diagonal = flip(beside, 2)

    def load(h):
        return pltpu.make_async_copy(states.at[:, h], held.at[h], load_sems.at[h])

    def first(i):
        return remote(own.at[i], mir.at[i], send_sems.at[0, i], recv_sems.at[0, i], device(across))

    def second(i):
        return remote(xsnd.at[i], xrcv.at[i], send_sems.at[1, i], recv_sems.at[1, i], device(beside))

    def third(i):
        return remote(zsnd.at[i], zrcv.at[i], send_sems.at[2, i], recv_sems.at[2, i], device(along))

    def note(j):
        return remote(mloc, mrcv.at[j], msend.at[j], mrecv.at[j], peer(j))

    def entry(j):
        return remote(esnd.at[j], ercv.at[j], esend.at[j], erecv.at[j], peer(n - j))

    def store(i):
        h, part = lax.div(i, SPLIT), pl.ds(lax.rem(i, SPLIT) * rows, rows)
        return pltpu.make_async_copy(fresh.at[i], new_states.at[:, h, part, :], store_sems.at[i])

    for h in range(heads):
        load(h).start()
    barrier = pltpu.get_barrier_semaphore()

    def greet(j):
        pl.semaphore_signal(barrier, inc=1, device_id={"beam": peer(j)}, device_id_type=MESH)

    repeat(1, n, greet)

    mloc[...] = jnp.zeros(mloc.shape, jnp.int32)
    for h in range(heads):
        mloc[:, h * hyps:(h + 1) * hyps] = token[...] * heads + h
    mloc[:, ids:ids + hyps] = parent[...]

    def encode_chunk(i):
        h, s = lax.div(i, SPLIT), lax.rem(i, SPLIT)

        @pl.when(s == 0)
        def _():
            load(h).wait()

        for u in range(hyps):
            own[i, u] = encode(held[h, u, pl.ds(s * rows, rows), :])

    repeat(0, AHEAD, encode_chunk)
    pl.semaphore_wait(barrier, n - 1)
    repeat(1, n, lambda j: note(j).start())
    for i in range(AHEAD):
        first(i).start()
    repeat(AHEAD, chunks, encode_chunk)
    mrcv[0] = mloc[...]
    repeat(1, n, lambda j: note(j).wait())

    spot = lax.broadcasted_iota(jnp.int32, (ids, vocab * heads), 1) + me * (vocab * heads)
    gate_spot = lax.broadcasted_iota(jnp.int32, (ids, vocab), 1) + me * vocab
    head_of = lax.broadcasted_iota(jnp.int32, (ids, 1), 0) // hyps
    head_lane = lax.broadcasted_iota(jnp.int32, (ids, heads), 1) == head_of
    lane = lax.broadcasted_iota(jnp.int32, (ids, d), 1)
    flat = table[...].reshape(vocab * heads, 5 * d)

    def find(j):
        key = jnp.broadcast_to(mrcv[j], (8, d)).T[0:ids, 0:1]
        hit = (key == spot).astype(jnp.float32).astype(jnp.bfloat16)
        esnd[j, :, 0:5 * d] = jnp.dot(hit, flat, preferred_element_type=jnp.float32).astype(jnp.bfloat16)
        word = (key - head_of == gate_spot * heads).astype(jnp.float32).astype(jnp.bfloat16)
        gates = jnp.zeros((ids, d), jnp.float32)
        for g in range(3):
            every = lax.dot_general(word, gate[g], (((1,), (1,)), ((), ())), preferred_element_type=jnp.float32)
            one = jnp.sum(jnp.where(head_lane, every, 0.0), axis=1, keepdims=True)
            gates = jnp.where(lane == g, one, gates)
        esnd[j, :, 5 * d:6 * d] = gates.astype(jnp.bfloat16)

        @pl.when(j > 0)
        def _():
            entry(j).start()

    repeat(0, n, find)

    place = lax.broadcasted_iota(jnp.int32, (1, d), 1)

    def parents_of(b):
        row = mrcv[lax.rem(me - device(b) + n, n)]
        return [jnp.broadcast_to(jnp.sum(jnp.where(place == ids + u, row, 0), axis=1, keepdims=True), (1, d)) for u in range(hyps)]

    mine = parents_of(beam)
    at_beside, at_diagonal, at_along = parents_of(beside), parents_of(diagonal), parents_of(along)

    def wide(code):
        return code.astype(jnp.int32)

    out_lane = lax.broadcasted_iota(jnp.int32, (rows, d), 1)
    outs[...] = jnp.zeros(outs.shape, jnp.float32)

    def prepare():
        def add(j, total):
            entry(j).wait_recv()
            return total + ercv[j].astype(jnp.float32)

        total = lax.fori_loop(1, n, add, esnd[0].astype(jnp.float32))
        for part in range(3):
            keys[part] = unit_norm(total[:, part * d:(part + 1) * d])
        sigmoids = jax.nn.sigmoid(total[:, 5 * d:6 * d])
        for g in range(3):
            strengths[g] = jnp.broadcast_to(sigmoids[:, g:g + 1] * (1.0 if g == 0 else 2.0), (ids, d))
        for j in range(2):
            value = total[:, (3 + j) * d:(4 + j) * d].T
            for h in range(heads):
                for s in range(SPLIT):
                    columns[j, h * SPLIT + s, :, 0:hyps] = value[s * rows:(s + 1) * rows, h * hyps:(h + 1) * hyps]

    def advance(i):
        @pl.when(i < chunks)
        def _():
            first(i).wait_recv()

            @pl.when(i + AHEAD < chunks)
            def _():
                first(i + AHEAD).start()

            for u in range(hyps):
                a, m = wide(own[i, u]), wide(mir[i, u])
                xsnd[i, u] = jnp.where(at_beside[u] == beam, a, m).astype(jnp.int16)
                xsnd[i, hyps + u] = jnp.where(at_diagonal[u] == beam, a, m).astype(jnp.int16)
            second(i).start()

        t = i - LAG

        @pl.when((t >= 0) & (t < chunks))
        def _():
            second(t).wait_recv()
            for u in range(hyps):
                a, m, x = wide(own[t, u]), wide(mir[t, u]), wide(xrcv[t, hyps + u])
                p = at_along[u]
                zsnd[t, u] = jnp.where(p == beam, a, jnp.where(p == across, m, x)).astype(jnp.int16)
            third(t).start()

        f = i - 2 * LAG

        @pl.when(f == 0)
        def _():
            prepare()

        @pl.when(f >= 0)
        def _():
            h, s = lax.div(f, SPLIT), lax.rem(f, SPLIT)
            third(f).wait_recv()
            for u in range(hyps):
                m, x, z = wide(mir[f, u]), wide(xrcv[f, u]), wide(zrcv[f, u])
                p = mine[u]
                near = (p == beside) | (p == flip(beside, 4))
                got = decode(jnp.where(p == across, m, jnp.where(near, x, z)))
                row = pl.ds(h * hyps + u, 1)
                now = strengths[0, row, :] * jnp.where(p == beam, held[h, u, pl.ds(s * rows, rows), :], got)
                for j in range(2):
                    key = keys[1 + j, row, :]
                    applied = jnp.sum(now * key, axis=1, keepdims=True)
                    now = now - (applied - columns[j, f, :, u:u + 1]) * (strengths[1 + j, row, :] * key)
                fresh[f, u] = now
                out = jnp.sum(now * keys[0, row, :], axis=1, keepdims=True)
                outs[s] = jnp.where(out_lane == h * hyps + u, out, outs[s])
            store(f).start()

    repeat(0, chunks + 2 * LAG, advance)

    out_rows = outs[...].reshape(d, d).T[0:ids]
    out_rows = out_rows * lax.rsqrt(jnp.mean(out_rows * out_rows, axis=-1, keepdims=True) + 1e-05)
    for h in range(heads):
        for u in range(hyps):
            k = h * hyps + u
            readout[u, h:h + 1, :] = (gain[h:h + 1, :] * out_rows[k:k + 1, :]).astype(jnp.bfloat16)
    repeat(1, n, lambda j: entry(j).wait_send())

    def finish(i):
        first(i).wait_send()
        second(i).wait_send()
        third(i).wait_send()
        store(i).wait()

    repeat(0, chunks, finish)


def local(states, parent_beam, next_token, proj_table, gate_table, gain):
    hyps, heads = states.shape[:2]
    vocab = proj_table.shape[0]
    n = lax.axis_size("beam")
    ids = hyps * heads
    chunks, rows = heads * SPLIT, HEAD_DIM // SPLIT
    width = 6 * HEAD_DIM
    vmem = pl.BlockSpec(memory_space=pltpu.VMEM)
    hbm = pl.BlockSpec(memory_space=pl.ANY)

    def codes(slots):
        return pltpu.VMEM((chunks, slots, rows, HEAD_DIM), jnp.int16)

    dma = pltpu.SemaphoreType.DMA
    return pl.pallas_call(
        lambda *refs: step_kernel(n, heads, hyps, vocab, *refs),
        out_shape=(
            jax.ShapeDtypeStruct((hyps, heads, HEAD_DIM), jnp.bfloat16),
            jax.ShapeDtypeStruct(states.shape, jnp.float32),
        ),
        in_specs=[hbm] + [vmem] * 5,
        out_specs=(vmem, hbm),
        scratch_shapes=[
            pltpu.VMEM((heads, hyps, HEAD_DIM, HEAD_DIM), jnp.float32),
            codes(hyps), codes(hyps), codes(2 * hyps), codes(2 * hyps), codes(hyps), codes(hyps),
            pltpu.VMEM((1, HEAD_DIM), jnp.int32),
            pltpu.VMEM((n, 1, HEAD_DIM), jnp.int32),
            pltpu.VMEM((n, ids, width), jnp.bfloat16),
            pltpu.VMEM((n, ids, width), jnp.bfloat16),
            pltpu.VMEM((chunks, hyps, rows, HEAD_DIM), jnp.float32),
            pltpu.VMEM((3, ids, HEAD_DIM), jnp.float32),
            pltpu.VMEM((2, chunks, rows, HEAD_DIM), jnp.float32),
            pltpu.VMEM((3, ids, HEAD_DIM), jnp.float32),
            pltpu.VMEM((SPLIT, rows, HEAD_DIM), jnp.float32),
            dma((3, chunks)), dma((3, chunks)), dma((n,)), dma((n,)), dma((n,)), dma((n,)),
            dma((heads,)), dma((chunks,)),
        ],
        compiler_params=pltpu.CompilerParams(collective_id=0, has_side_effects=True),
        name="step",
    )(
        states, next_token.reshape(1, hyps), parent_beam.reshape(1, hyps), proj_table,
        jnp.transpose(gate_table, (1, 2, 0)), gain,
    )


def solution(mesh):
    return jax.shard_map(
        local,
        mesh=mesh,
        in_specs=(
            P(("groups", "beam"), "mp", None, None),
            P(("groups", "beam")),
            P(("groups", "beam")),
            P("beam", "mp", None),
            P("beam", None, "mp"),
            P("mp", None),
        ),
        out_specs=(P(("groups", "beam"), "mp", None), P(("groups", "beam"), "mp", None, None)),
        check_vma=False,
    )
```

```python
import jax
import jax.numpy as jnp
from jax import lax
from jax.experimental import pallas as pl
from jax.experimental.pallas import tpu as pltpu
from jax.sharding import PartitionSpec as P

HEAD_DIM = 128
BEAMS = 8
SPLIT = 2
AHEAD = 3
LAG = 2
LATE = 7
PEAK = 4.0
LEVELS = 32767.0
MESH = pl.DeviceIdType.MESH


def encode(x):
    root = jnp.sqrt(jnp.sqrt(jnp.sqrt(jnp.abs(x) * (1.0 / PEAK))))
    scaled = jnp.where(x < 0, -root, root) * LEVELS
    return jnp.round(scaled).astype(jnp.int32).astype(jnp.int16)


def decode(code):
    y = code.astype(jnp.int32).astype(jnp.float32) * (1.0 / LEVELS)
    y2 = y * y
    y4 = y2 * y2
    return (y4 * PEAK) * (y4 * jnp.where(y < 0, -1.0, 1.0))


def flip(beam, bit):
    return beam + bit - 2 * bit * lax.rem(lax.div(beam, bit), 2)


def unit_norm(vector):
    return vector * lax.rsqrt(jnp.sum(vector * vector, axis=-1, keepdims=True) + 1e-06)


def step_kernel(
    n, heads, hyps, vocab, states, token, parent, table_home, gate, gain, readout, new_states,
    held, own, mir, xsnd, xrcv, zsnd, zrcv, mloc, mrcv, esnd, ercv, fresh,
    keys, columns, strengths, outs, table, table_sem,
    send_sems, recv_sems, msend, mrecv, esend, erecv, load_sems, store_sems,
):
    me = lax.axis_index("beam")
    spacing = n // BEAMS
    beam = lax.div(me, spacing)
    off = lax.rem(me, spacing)
    d = HEAD_DIM
    chunks = heads * SPLIT
    rows = d // SPLIT
    ids = hyps * heads

    def device(b):
        return b * spacing + off

    def peer(j):
        return lax.rem(me + j, n)

    def repeat(low, high, body):
        def step(i, carry):
            body(i)
            return carry
        lax.fori_loop(low, high, step, 0)

    def remote(src, dst, send, recv, to):
        return pltpu.make_async_remote_copy(
            src_ref=src, dst_ref=dst, send_sem=send, recv_sem=recv,
            device_id={"beam": to}, device_id_type=MESH,
        )

    across, beside, along = flip(beam, 4), flip(beam, 1), flip(beam, 2)
    diagonal = flip(beside, 2)

    def load(h):
        return pltpu.make_async_copy(states.at[:, h], held.at[h], load_sems.at[h])

    def first(i):
        return remote(own.at[i], mir.at[i], send_sems.at[0, i], recv_sems.at[0, i], device(across))

    def second(i):
        return remote(xsnd.at[i], xrcv.at[i], send_sems.at[1, i], recv_sems.at[1, i], device(beside))

    def third(i):
        return remote(zsnd.at[i], zrcv.at[i], send_sems.at[2, i], recv_sems.at[2, i], device(along))

    def note(j):
        return remote(mloc, mrcv.at[j], msend.at[j], mrecv.at[j], peer(j))

    def entry(j):
        return remote(esnd.at[j], ercv.at[j], esend.at[j], erecv.at[j], peer(n - j))

    def store(i):
        h, part = lax.div(i, SPLIT), pl.ds(lax.rem(i, SPLIT) * rows, rows)
        return pltpu.make_async_copy(fresh.at[i], new_states.at[:, h, part, :], store_sems.at[i])

    for h in range(heads):
        load(h).start()
    table_load = pltpu.make_async_copy(table_home, table, table_sem)
    table_load.start()
    barrier = pltpu.get_barrier_semaphore()

    def greet(j):
        pl.semaphore_signal(barrier, inc=1, device_id={"beam": peer(j)}, device_id_type=MESH)

    repeat(1, n, greet)

    mloc[...] = jnp.zeros(mloc.shape, jnp.int32)
    for h in range(heads):
        mloc[:, h * hyps:(h + 1) * hyps] = token[...] * heads + h
    mloc[:, ids:ids + hyps] = parent[...]

    def encode_chunk(i):
        h, s = lax.div(i, SPLIT), lax.rem(i, SPLIT)

        @pl.when(s == 0)
        def _():
            load(h).wait()

        for u in range(hyps):
            own[i, u] = encode(held[h, u, pl.ds(s * rows, rows), :])

    repeat(0, AHEAD, encode_chunk)
    pl.semaphore_wait(barrier, n - 1)
    repeat(1, n, lambda j: note(j).start())
    for i in range(AHEAD):
        first(i).start()
    repeat(AHEAD, chunks, encode_chunk)
    mrcv[0] = mloc[...]
    repeat(1, n, lambda j: note(j).wait())

    spot = lax.broadcasted_iota(jnp.int32, (ids, vocab * heads), 1) + me * (vocab * heads)
    gate_spot = lax.broadcasted_iota(jnp.int32, (ids, vocab), 1) + me * vocab
    head_of = lax.broadcasted_iota(jnp.int32, (ids, 1), 0) // hyps
    head_lane = lax.broadcasted_iota(jnp.int32, (ids, heads), 1) == head_of
    lane = lax.broadcasted_iota(jnp.int32, (ids, d), 1)
    table_load.wait()
    flat = table[...].reshape(vocab * heads, 5 * d)

    def find(j):
        key = jnp.broadcast_to(mrcv[j], (8, d)).T[0:ids, 0:1]
        hit = (key == spot).astype(jnp.float32).astype(jnp.bfloat16)
        esnd[j, :, 0:5 * d] = jnp.dot(hit, flat, preferred_element_type=jnp.float32).astype(jnp.bfloat16)
        word = (key - head_of == gate_spot * heads).astype(jnp.float32).astype(jnp.bfloat16)
        gates = jnp.zeros((ids, d), jnp.float32)
        for g in range(3):
            every = lax.dot_general(word, gate[g], (((1,), (1,)), ((), ())), preferred_element_type=jnp.float32)
            one = jnp.sum(jnp.where(head_lane, every, 0.0), axis=1, keepdims=True)
            gates = jnp.where(lane == g, one, gates)
        esnd[j, :, 5 * d:6 * d] = gates.astype(jnp.bfloat16)

    repeat(0, n, find)

    place = lax.broadcasted_iota(jnp.int32, (1, d), 1)

    def parents_of(b):
        row = mrcv[lax.rem(me - device(b) + n, n)]
        return [jnp.broadcast_to(jnp.sum(jnp.where(place == ids + u, row, 0), axis=1, keepdims=True), (1, d)) for u in range(hyps)]

    mine = parents_of(beam)
    at_beside, at_diagonal, at_along = parents_of(beside), parents_of(diagonal), parents_of(along)

    def wide(code):
        return code.astype(jnp.int32)

    out_lane = lax.broadcasted_iota(jnp.int32, (rows, d), 1)
    outs[...] = jnp.zeros(outs.shape, jnp.float32)

    def prepare():
        def add(j, total):
            entry(j).wait_recv()
            return total + ercv[j].astype(jnp.float32)

        total = lax.fori_loop(1, n, add, esnd[0].astype(jnp.float32))
        for part in range(3):
            keys[part] = unit_norm(total[:, part * d:(part + 1) * d])
        sigmoids = jax.nn.sigmoid(total[:, 5 * d:6 * d])
        for g in range(3):
            strengths[g] = jnp.broadcast_to(sigmoids[:, g:g + 1] * (1.0 if g == 0 else 2.0), (ids, d))
        for j in range(2):
            value = total[:, (3 + j) * d:(4 + j) * d].T
            for h in range(heads):
                for s in range(SPLIT):
                    columns[j, h * SPLIT + s, :, 0:hyps] = value[s * rows:(s + 1) * rows, h * hyps:(h + 1) * hyps]

    def advance(i):
        @pl.when(i < chunks)
        def _():
            first(i).wait_recv()

            @pl.when(i + AHEAD < chunks)
            def _():
                first(i + AHEAD).start()

            for u in range(hyps):
                a, m = wide(own[i, u]), wide(mir[i, u])
                xsnd[i, u] = jnp.where(at_beside[u] == beam, a, m).astype(jnp.int16)
                xsnd[i, hyps + u] = jnp.where(at_diagonal[u] == beam, a, m).astype(jnp.int16)
            second(i).start()

        @pl.when(i == chunks - AHEAD)
        def _():
            repeat(1, n, lambda j: entry(j).start())

        t = i - LAG

        @pl.when((t >= 0) & (t < chunks))
        def _():
            second(t).wait_recv()
            for u in range(hyps):
                a, m, x = wide(own[t, u]), wide(mir[t, u]), wide(xrcv[t, hyps + u])
                p = at_along[u]
                zsnd[t, u] = jnp.where(p == beam, a, jnp.where(p == across, m, x)).astype(jnp.int16)
            third(t).start()

        f = i - LATE

        @pl.when(f == 0)
        def _():
            prepare()

        @pl.when(f >= 0)
        def _():
            h, s = lax.div(f, SPLIT), lax.rem(f, SPLIT)
            third(f).wait_recv()
            for u in range(hyps):
                m, x, z = wide(mir[f, u]), wide(xrcv[f, u]), wide(zrcv[f, u])
                p = mine[u]
                near = (p == beside) | (p == flip(beside, 4))
                got = decode(jnp.where(p == across, m, jnp.where(near, x, z)))
                row = pl.ds(h * hyps + u, 1)
                now = strengths[0, row, :] * jnp.where(p == beam, held[h, u, pl.ds(s * rows, rows), :], got)
                for j in range(2):
                    key = keys[1 + j, row, :]
                    applied = jnp.sum(now * key, axis=1, keepdims=True)
                    now = now - (applied - columns[j, f, :, u:u + 1]) * (strengths[1 + j, row, :] * key)
                fresh[f, u] = now
                out = jnp.sum(now * keys[0, row, :], axis=1, keepdims=True)
                outs[s] = jnp.where(out_lane == h * hyps + u, out, outs[s])
            store(f).start()

    repeat(0, chunks + LATE, advance)

    out_rows = outs[...].reshape(d, d).T[0:ids]
    out_rows = out_rows * lax.rsqrt(jnp.mean(out_rows * out_rows, axis=-1, keepdims=True) + 1e-05)
    for h in range(heads):
        for u in range(hyps):
            k = h * hyps + u
            readout[u, h:h + 1, :] = (gain[h:h + 1, :] * out_rows[k:k + 1, :]).astype(jnp.bfloat16)
    repeat(1, n, lambda j: entry(j).wait_send())

    def finish(i):
        first(i).wait_send()
        second(i).wait_send()
        third(i).wait_send()
        store(i).wait()

    repeat(0, chunks, finish)


def place_kernel(hyps, rows_in, states_in, rows_out, states_out, held, loads, stores):
    rows_out[...] = rows_in[...]
    ins = [pltpu.make_async_copy(states_in.at[u], held.at[u], loads.at[u]) for u in range(hyps)]
    outs = [pltpu.make_async_copy(held.at[u], states_out.at[u], stores.at[u]) for u in range(hyps)]
    for c in ins:
        c.start()
    for u in range(hyps):
        ins[u].wait()
        outs[u].start()
    for c in outs:
        c.wait()


def local(states, parent_beam, next_token, proj_table, gate_table, gain):
    hyps, heads = states.shape[:2]
    vocab = proj_table.shape[0]
    n = lax.axis_size("beam")
    ids = hyps * heads
    chunks, rows = heads * SPLIT, HEAD_DIM // SPLIT
    width = 6 * HEAD_DIM
    vmem = pl.BlockSpec(memory_space=pltpu.VMEM)
    hbm = pl.BlockSpec(memory_space=pl.ANY)

    def codes(slots):
        return pltpu.VMEM((chunks, slots, rows, HEAD_DIM), jnp.int16)

    dma = pltpu.SemaphoreType.DMA
    result = pl.pallas_call(
        lambda *refs: step_kernel(n, heads, hyps, vocab, *refs),
        out_shape=(
            jax.ShapeDtypeStruct((hyps, heads, HEAD_DIM), jnp.bfloat16),
            jax.ShapeDtypeStruct(states.shape, jnp.float32),
        ),
        in_specs=[hbm, vmem, vmem, hbm, vmem, vmem],
        out_specs=(vmem, hbm),
        scratch_shapes=[
            pltpu.VMEM((heads, hyps, HEAD_DIM, HEAD_DIM), jnp.float32),
            codes(hyps), codes(hyps), codes(2 * hyps), codes(2 * hyps), codes(hyps), codes(hyps),
            pltpu.VMEM((1, HEAD_DIM), jnp.int32),
            pltpu.VMEM((n, 1, HEAD_DIM), jnp.int32),
            pltpu.VMEM((n, ids, width), jnp.bfloat16),
            pltpu.VMEM((n, ids, width), jnp.bfloat16),
            pltpu.VMEM((chunks, hyps, rows, HEAD_DIM), jnp.float32),
            pltpu.VMEM((3, ids, HEAD_DIM), jnp.float32),
            pltpu.VMEM((2, chunks, rows, HEAD_DIM), jnp.float32),
            pltpu.VMEM((3, ids, HEAD_DIM), jnp.float32),
            pltpu.VMEM((SPLIT, rows, HEAD_DIM), jnp.float32),
            pltpu.VMEM(proj_table.shape, proj_table.dtype),
            dma,
            dma((3, chunks)), dma((3, chunks)), dma((n,)), dma((n,)), dma((n,)), dma((n,)),
            dma((heads,)), dma((chunks,)),
        ],
        compiler_params=pltpu.CompilerParams(collective_id=0, has_side_effects=True),
        name="step",
    )(
        states, next_token.reshape(1, hyps), parent_beam.reshape(1, hyps), proj_table,
        jnp.transpose(gate_table, (1, 2, 0)), gain,
    )
    return pl.pallas_call(
        lambda *refs: place_kernel(hyps, *refs),
        out_shape=tuple(jax.ShapeDtypeStruct(r.shape, r.dtype) for r in result),
        in_specs=[vmem, hbm],
        out_specs=(vmem, hbm),
        scratch_shapes=[pltpu.VMEM(states.shape, states.dtype), dma((hyps,)), dma((hyps,))],
        name="place",
    )(*result)


def solution(mesh):
    return jax.shard_map(
        local,
        mesh=mesh,
        in_specs=(
            P(("groups", "beam"), "mp", None, None),
            P(("groups", "beam")),
            P(("groups", "beam")),
            P("beam", "mp", None),
            P("beam", None, "mp"),
            P("mp", None),
        ),
        out_specs=(P(("groups", "beam"), "mp", None), P(("groups", "beam"), "mp", None, None)),
        check_vma=False,
    )
```
